32 devices in a mesh: replica: 4 (over y, core), fsdp: 8 (over z, x).
Axes of the slice: x: 2, y: 2, z: 4, core: 2. Of those that a mesh axis runs over, the one named last changes fastest.
Arguments:
- hidden_states: bfloat16 [4, 2048, 4096], P('replica', 'fsdp'), may hold values from -6 to 6
- norm_gain: bfloat16 [4, 4096], P('replica', 'fsdp'), may hold values from 0.5 to 1.5
- key_weight: bfloat16 [4, 4096, 1024], P('replica', 'fsdp'), may hold values from -0.09375 to 0.09375
- value_weight: bfloat16 [4, 4096, 1024], P('replica', 'fsdp'), may hold values from -0.09375 to 0.09375
- deltas: float32 [4, 256, 4096], P('replica', 'fsdp'), may hold values from -6 to 6
- outer_params: float32 [256, 4096], P('fsdp', 'replica'), may hold values from -6 to 6
- momentum: float32 [256, 4096], P('fsdp', 'replica'), may hold values from -3 to 3
- local_params: bfloat16 [4, 256, 4096], P('replica', 'fsdp'), may hold values from -6 to 6
Outputs:
- keys: bfloat16 [4, 2048, 1024], P('replica', 'fsdp')
- values: bfloat16 [4, 2048, 1024], P('replica', 'fsdp')
- momentum_new: float32 [256, 4096], P('fsdp', 'replica')
- outer_new: float32 [256, 4096], P('fsdp', 'replica')
- local_new: bfloat16 [4, 256, 4096], P('replica', 'fsdp')
The draws below stay inside these ranges and needn't reach their ends.
All inputs are finite; a program needn't handle non-finite values.
Results may differ from the reference program's by a relative error of at most 0.0085.
Values may be sent and summed in bfloat16 or wider, within the bound.
A program may use at most 128 MiB of HBM per device.

```python
import jax
import jax.numpy as jnp
from jax import lax

D = 4096
HEAD = 128
KV = 1024
TOK_DEV = 256
TOKENS_R = 2048
FRAG_ROWS = 256
N_REPLICA = 4


def raised(entries, key, source, target, parts, factor):
    def block_of(axis_at):
        return (jnp.arange(entries.shape[axis_at]) // (entries.shape[axis_at] // parts)).reshape((-1,) + (1,) * (entries.ndim - 1 - axis_at))

    one_side = jax.random.permutation(key, parts)[block_of(target)]
    second = (block_of(target) + parts // 2) % parts
    return jnp.where((block_of(source) == one_side) | (block_of(source) == second), factor * entries, entries)


def levels(rng, extent, pieces, smallest, high):
    loudness = 1.0
    for position, shards_of in pieces:
        draws = jax.random.uniform(jax.random.fold_in(jax.random.fold_in(rng, 6), position), (shards_of,), jnp.float32, smallest / len(pieces), high / len(pieces))
        loudness = loudness * jnp.repeat(jnp.exp(draws), extent[position] // shards_of).reshape((-1,) + (1,) * (len(extent) - 1 - position))
    return loudness


def bell_draw(key, dims, deviation, reach, shards=(), held_as=jnp.bfloat16):
    values = deviation * jax.random.normal(key, dims, jnp.float32)
    if shards:
        values = values * levels(key, dims, shards, -0.22, 0.18)
    return jnp.clip(values, -reach, reach).astype(held_as)


def heavy_noise(stream_key, shape, scale, most, shards, heavy, kind=jnp.bfloat16):
    result = scale * jax.random.normal(stream_key, shape, jnp.float32)
    if shards:
        result = result * levels(stream_key, shape, shards, -0.22, 0.18)
    return jnp.clip(raised(result, jax.random.fold_in(stream_key, 3), *heavy), -most, most).astype(kind)


def setup_inputs(seed: int = 0) -> dict:
    key_list = jax.random.split(jax.random.key(seed), 9)
    return {
        "hidden_states": bell_draw(key_list[0], (N_REPLICA, TOKENS_R, D), 1.0, 6.0, ((0, 4), (1, 8))),
        "norm_gain": jnp.clip(1.0 + 0.1 * jax.random.normal(key_list[1], (N_REPLICA, D), jnp.float32), 0.5, 1.5).astype(jnp.bfloat16),
        "key_weight": bell_draw(key_list[2], (N_REPLICA, D, KV), D ** -0.5, 0.09375, ((0, 4), (1, 8))),
        "value_weight": bell_draw(key_list[3], (N_REPLICA, D, KV), D ** -0.5, 0.09375, ((0, 4), (1, 8))),
        "deltas": heavy_noise(key_list[4], (N_REPLICA, FRAG_ROWS, D), 1.0, 6.0, ((0, 4), (1, 8)), (0, 2, 4, 2.0), jnp.float32),
        "outer_params": bell_draw(key_list[5], (FRAG_ROWS, D), 1.0, 6.0, ((0, 8), (1, 4)), jnp.float32),
        "momentum": bell_draw(key_list[6], (FRAG_ROWS, D), 0.5, 3.0, ((0, 8), (1, 4)), jnp.float32),
        "local_params": bell_draw(key_list[7], (N_REPLICA, FRAG_ROWS, D), 1.0, 6.0, ((0, 4), (1, 8))),
    }


def rotate_keys(keys_raw, positions, head_size):
    half_width = head_size // 2
    exponent = jnp.arange(half_width, dtype=jnp.float32) * (2.0 / head_size)
    frequency = jnp.power(jnp.float32(500000.0), -exponent)
    angles = positions.astype(jnp.float32)[:, None] * frequency[None, :]
    cosine_table = jnp.cos(angles)[:, None, :]
    sine_table = jnp.sin(angles)[:, None, :]
    shaped = keys_raw.reshape(keys_raw.shape[0], -1, head_size)
    first_half = shaped[:, :, :half_width]
    second_half = shaped[:, :, half_width:]
    turned = jnp.concatenate([first_half * cosine_table - second_half * sine_table, second_half * cosine_table + first_half * sine_table], axis=2)
    return turned.reshape(keys_raw.shape)

def project_replica(inputs):
    states, gain, weight_key, weight_value = inputs
    states32 = states.astype(jnp.float32)
    inv_rms = lax.rsqrt(lax.optimization_barrier(jnp.mean(states32 * states32, axis=1, keepdims=True)) + 1e-05)
    normed = (states32 * inv_rms * gain.astype(jnp.float32)[None, :]).astype(jnp.bfloat16)
    keys_raw = jnp.dot(normed, weight_key, preferred_element_type=jnp.float32)
    values_raw = jnp.dot(normed, weight_value, preferred_element_type=jnp.float32)
    positions = jnp.arange(states.shape[0], dtype=jnp.int32) % TOK_DEV
    rotated = rotate_keys(keys_raw, positions, HEAD)
    return (rotated.astype(jnp.bfloat16), values_raw.astype(jnp.bfloat16))

def reference(hidden_states, norm_gain, key_weight, value_weight, deltas, outer_params, momentum, local_params):
    keys, values = lax.map(project_replica, (hidden_states, norm_gain, key_weight, value_weight))
    avg_delta = lax.optimization_barrier(jnp.sum(deltas, axis=0)) / deltas.shape[0]
    momentum_new = 0.9 * momentum + avg_delta
    outer_new = outer_params - 0.7 * (avg_delta + 0.9 * momentum_new)
    local_new = (0.5 * local_params.astype(jnp.float32) + 0.5 * outer_new[None, :, :]).astype(jnp.bfloat16)
    return (keys, values, momentum_new, outer_new, local_new)
```

```python
import functools

import jax
import jax.numpy as jnp
from jax import lax
from jax.experimental import pallas as pl
from jax.experimental.pallas import tpu as pltpu
from jax.sharding import PartitionSpec as P

HEAD = 128
MESH = pl.DeviceIdType.MESH


def rotation_tables(tokens, head_size):
    half_width = head_size // 2
    exponent = jnp.arange(half_width, dtype=jnp.float32) * (2.0 / head_size)
    frequency = jnp.power(jnp.float32(500000.0), -exponent)
    angles = jnp.arange(tokens, dtype=jnp.int32).astype(jnp.float32)[:, None] * frequency[None, :]
    cosine, sine = jnp.cos(angles), jnp.sin(angles)
    return jnp.concatenate([cosine, cosine], axis=1), jnp.concatenate([-sine, sine], axis=1)


def stage_plan(groups):
    plan, left, bit = [], list(range(groups)), 1
    while bit < groups:
        plan.append((bit, [b for b in left if b & bit], [b for b in left if not b & bit]))
        left = plan[-1][2]
        bit *= 2
    return plan


def kernel(
    groups, replicas, width,
    hs, gain, kw, vw, cosine, sine, deltas, outer, momentum, local,
    keys, values, momentum_new, outer_new, local_new,
    hs_v, gains, a_in, a_scaled, weights, inv, partial, d_in, o_in, *rest,
):
    plan = stage_plan(groups)
    stages = len(plan)
    c_out, c_in, rest = rest[:stages], rest[stages : 2 * stages], rest[2 * stages :]
    hs_sem, g_sem, a_sem, b_sem, own_sem, c_sem, d_sem, o_sem = rest

    r, f = lax.axis_index("replica"), lax.axis_index("fsdp")
    x, z = lax.rem(f, 2), lax.div(f, 2)
    tokens, depth = hs.shape[0], kw.shape[0]
    quarter = 2 * depth
    per_weight = kw.shape[1] // width
    chunks = 2 * per_weight
    own_w = outer.shape[1]

    def group_at(offset):
        g, bit = z, 1
        while bit < groups:
            if offset & bit:
                g = g + bit * (1 - 2 * lax.rem(lax.div(g, bit), 2))
            bit *= 2
        return g

    def peer(offset):
        return {"fsdp": 2 * group_at(offset) + x}

    partner = {"fsdp": f + 1 - 2 * x}

    def replica_at(j):
        return lax.rem(r + j, replicas)

    barrier = pltpu.get_barrier_semaphore()
    pl.semaphore_signal(barrier, inc=1, device_id=partner, device_id_type=MESH)
    for b in range(1, groups):
        pl.semaphore_signal(barrier, inc=1, device_id=peer(b), device_id_type=MESH)
    for j in range(1, replicas):
        pl.semaphore_signal(
            barrier, inc=1, device_id={"replica": replica_at(j)}, device_id_type=MESH
        )

    def remote(src, dst, sems, index, target):
        return pltpu.make_async_remote_copy(
            src_ref=src, dst_ref=dst, send_sem=sems.at[(0,) + index],
            recv_sem=sems.at[(1,) + index], device_id=target, device_id_type=MESH,
        )

    hs_copy = pltpu.make_async_copy(hs, hs_v, hs_sem)
    hs_copy.start()
    rows = pl.ds(pl.multiple_of(x * depth, depth), depth)
    own_copies = []
    for c in range(chunks):
        source = (kw if c < per_weight else vw).at[:, pl.ds((c % per_weight) * width, width)]
        own_copies.append(pltpu.make_async_copy(source, weights.at[c, rows], own_sem.at[c]))
        own_copies[-1].start()

    pl.semaphore_wait(barrier, groups + replicas - 1)

    gain_copy = remote(gain, gains.at[x], g_sem, (), partner)
    gain_copy.start()
    a_copies = {}
    order = plan[0][1] + [b for b in plan[0][2] if b]
    for b in order:
        columns = pl.ds(pl.multiple_of(group_at(b) * quarter, quarter), quarter)
        a_copies[b] = remote(hs.at[:, columns], a_in.at[b - 1], a_sem, (b - 1,), peer(b))
        a_copies[b].start()
    b_copies = []
    for c in range(chunks):
        source = (kw if c < per_weight else vw).at[:, pl.ds((c % per_weight) * width, width)]
        b_copies.append(remote(source, weights.at[c, rows], b_sem, (c,), partner))
        b_copies[-1].start()
    d_copies = []
    for j in range(1, replicas):
        columns = pl.ds(pl.multiple_of(replica_at(j) * own_w, own_w), own_w)
        d_copies.append(
            remote(
                deltas.at[:, columns], d_in.at[j - 1], d_sem, (j - 1,), {"replica": replica_at(j)}
            )
        )
        d_copies[-1].start()

    def c_copy(stage, c):
        return remote(
            c_out[stage].at[c], c_in[stage].at[c], c_sem, (stage, c), peer(plan[stage][0])
        )

    def b_wait(c):
        pltpu.make_async_copy(
            kw.at[:, pl.ds(0, width)], weights.at[c, rows], own_sem.at[c]
        ).wait()
        remote(
            kw.at[:, pl.ds(0, width)], weights.at[c, rows], b_sem, (c,), partner
        ).wait_recv()

    hs_copy.wait()
    total = jnp.zeros((tokens, 1), jnp.float32)
    features = hs.shape[1]
    for k in range(groups):
        part = hs_v[:, k * quarter : (k + 1) * quarter].astype(jnp.float32)
        total += jnp.sum(part * part, axis=1, keepdims=True)
    inv[...] = jnp.broadcast_to(lax.rsqrt(total / features + 1e-05), inv.shape)

    gains[x] = gain[...]
    gain_copy.wait()
    gain_row = jnp.concatenate([gains[0], gains[1]], axis=1)

    def scale(b, block):
        a_scaled[b] = (block.astype(jnp.float32) * gain_row).astype(jnp.bfloat16)

    scale(0, hs_v[:, pl.ds(pl.multiple_of(z * quarter, quarter), quarter)])
    for b in plan[0][1]:
        a_copies[b].wait_recv()
        scale(b, a_in[b - 1])

    def product(b, c):
        return jnp.dot(a_scaled[b], weights[c], preferred_element_type=jnp.float32)

    @pl.loop(0, chunks)
    def _(c):
        b_wait(c)
        for i, b in enumerate(plan[0][1]):
            c_out[0][c, i] = product(b, c).astype(jnp.bfloat16)
        c_copy(0, c).start()

    avg = deltas[:, pl.ds(pl.multiple_of(r * own_w, own_w), own_w)]
    for j in range(1, replicas):
        d_copies[j - 1].wait_recv()
        avg += d_in[j - 1]
    avg = avg / replicas
    moved = 0.9 * momentum[...] + avg
    momentum_new[...] = moved
    outer_new[...] = outer[...] - 0.7 * (avg + 0.9 * moved)

    for b in plan[0][2]:
        if b:
            a_copies[b].wait_recv()
            scale(b, a_in[b - 1])

    o_copies = []
    for j in range(1, replicas):
        o_copies.append(
            remote(outer_new, o_in.at[j - 1], o_sem, (j - 1,), {"replica": replica_at(j)})
        )
        o_copies[-1].start()

    for stage in range(stages):
        bit, sent, kept = plan[stage]
        last = stage == stages - 1
        upcoming = [] if last else plan[stage + 1][1]

        def summed(b, c):
            before = product(b, c) if stage == 0 else partial[b, c]
            return before + c_in[stage][c, sent.index(b + bit)].astype(jnp.float32)

        if not last:

            @pl.loop(0, chunks)
            def _(c):
                c_copy(stage, c).wait_recv()
                for b in kept:
                    value = summed(b, c)
                    if b in upcoming:
                        c_out[stage + 1][c, upcoming.index(b)] = value.astype(jnp.bfloat16)
                    else:
                        partial[b, c] = value
                c_copy(stage + 1, c).start()

        if stage == 0:
            half = jnp.float32(0.5)
            mine = pl.ds(pl.multiple_of(r * own_w, own_w), own_w)
            local_new[:, mine] = (
                half * local[:, mine].astype(jnp.float32) + half * outer_new[...]
            ).astype(jnp.bfloat16)
            for j in range(1, replicas):
                o_copies[j - 1].wait_recv()
                theirs = pl.ds(
                    pl.multiple_of(lax.rem(r + replicas - j, replicas) * own_w, own_w), own_w
                )
                local_new[:, theirs] = (
                    half * local[:, theirs].astype(jnp.float32) + half * o_in[j - 1]
                ).astype(jnp.bfloat16)

        if last:

            @pl.loop(0, per_weight)
            def _(c):
                c_copy(stage, c).wait_recv()
                value = summed(0, c) * inv[:, 0:1]
                for h in range(width // HEAD):
                    head = value[:, h * HEAD : (h + 1) * HEAD]
                    turned = head * cosine[...] + pltpu.roll(head, HEAD // 2, 1) * sine[...]
                    at = pl.ds(pl.multiple_of(c * width + h * HEAD, HEAD), HEAD)
                    keys[:, at] = turned.astype(jnp.bfloat16)

            @pl.loop(0, per_weight)
            def _(c):
                c_copy(stage, c + per_weight).wait_recv()
                value = summed(0, c + per_weight) * inv[:, 0:1]
                at = pl.ds(pl.multiple_of(c * width, width), width)
                values[:, at] = value.astype(jnp.bfloat16)

    for copy in list(a_copies.values()) + b_copies + d_copies + o_copies:
        copy.wait_send()
    for stage in range(stages):

        @pl.loop(0, chunks)
        def _(c):
            c_copy(stage, c).wait_send()


def per_device(
    groups, replicas,
    hidden_states, norm_gain, key_weight, value_weight, deltas, outer_params, momentum, local_params,
):
    hs, kw, vw = hidden_states[0], key_weight[0], value_weight[0]
    tokens, features = hs.shape
    depth, kv = kw.shape
    width = 2 * HEAD
    chunks = 2 * kv // width
    cosine, sine = rotation_tables(tokens, HEAD)
    plan = stage_plan(groups)
    blocks = [pltpu.VMEM((chunks, len(p[1]), tokens, width), jnp.bfloat16) for p in plan]
    own = outer_params.shape
    vmem = pl.BlockSpec(memory_space=pltpu.VMEM)
    hbm = pl.BlockSpec(memory_space=pl.ANY)
    dma = pltpu.SemaphoreType.DMA
    keys, values, momentum_new, outer_new, local_new = pl.pallas_call(
        functools.partial(kernel, groups, replicas, width),
        out_shape=(
            jax.ShapeDtypeStruct((tokens, kv), jnp.bfloat16),
            jax.ShapeDtypeStruct((tokens, kv), jnp.bfloat16),
            jax.ShapeDtypeStruct(own, jnp.float32),
            jax.ShapeDtypeStruct(own, jnp.float32),
            jax.ShapeDtypeStruct(local_params.shape[1:], jnp.bfloat16),
        ),
        in_specs=[hbm, vmem, hbm, hbm] + [vmem] * 6,
        out_specs=[vmem] * 5,
        scratch_shapes=[
            pltpu.VMEM((tokens, features), jnp.bfloat16),
            pltpu.VMEM((2, 1, depth), jnp.float32),
            pltpu.VMEM((groups - 1, tokens, 2 * depth), jnp.bfloat16),
            pltpu.VMEM((groups, tokens, 2 * depth), jnp.bfloat16),
            pltpu.VMEM((chunks, 2 * depth, width), jnp.bfloat16),
            pltpu.VMEM((tokens, HEAD), jnp.float32),
            pltpu.VMEM((max(p + 1 for p in plan[0][2] if not p & 2), chunks, tokens, width), jnp.float32),
            pltpu.VMEM((replicas - 1,) + own, jnp.float32),
            pltpu.VMEM((replicas - 1,) + own, jnp.float32),
            *blocks,
            *blocks,
            dma,
            dma((2,)),
            dma((2, groups - 1)),
            dma((2, chunks)),
            dma((chunks,)),
            dma((2, len(plan), chunks)),
            dma((2, replicas - 1)),
            dma((2, replicas - 1)),
        ],
        compiler_params=pltpu.CompilerParams(
            collective_id=0, has_side_effects=True, vmem_limit_bytes=60 * 1024 * 1024
        ),
    )(
        hs, norm_gain.astype(jnp.float32), kw, vw, cosine, sine,
        deltas[0], outer_params, momentum, local_params[0],
    )
    return keys[None], values[None], momentum_new, outer_new, local_new[None]


def solution(mesh):
    in_specs = (
        P("replica", "fsdp", None),
        P("replica", "fsdp"),
        P("replica", "fsdp", None),
        P("replica", "fsdp", None),
        P("replica", "fsdp", None),
        P("fsdp", "replica"),
        P("fsdp", "replica"),
        P("replica", "fsdp", None),
    )
    out_specs = (
        P("replica", "fsdp", None),
        P("replica", "fsdp", None),
        P("fsdp", "replica"),
        P("fsdp", "replica"),
        P("replica", "fsdp", None),
    )
    groups, replicas = mesh.shape["fsdp"] // 2, mesh.shape["replica"]
    return jax.shard_map(
        functools.partial(per_device, groups, replicas),
        mesh=mesh, in_specs=in_specs, out_specs=out_specs, check_vma=False,
    )
```

```python
import functools

import jax
import jax.numpy as jnp
import numpy as np
from jax import lax
from jax.experimental import pallas as pl
from jax.experimental.pallas import tpu as pltpu
from jax.sharding import PartitionSpec as P

HEAD = 128
MESH = pl.DeviceIdType.MESH


def rotation_tables(tokens, head_size):
    half_width = head_size // 2
    exponent = np.arange(half_width, dtype=np.float32) * np.float32(2.0 / head_size)
    frequency = np.power(np.float32(500000.0), -exponent)
    angles = np.arange(tokens, dtype=np.float32)[:, None] * frequency[None, :]
    cosine, sine = np.cos(angles), np.sin(angles)
    return (
        jnp.asarray(np.concatenate([cosine, cosine], axis=1)),
        jnp.asarray(np.concatenate([-sine, sine], axis=1)),
    )


def write_out(*refs):
    count = len(refs) // 2
    sems = refs[-1]
    copies = [
        pltpu.make_async_copy(refs[i], refs[count + i], sems.at[i]) for i in range(count)
    ]
    for copy in copies:
        copy.start()
    for copy in copies:
        copy.wait()


def stage_plan(groups):
    plan, left, bit = [], list(range(groups)), 1
    while bit < groups:
        plan.append((bit, [b for b in left if b & bit], [b for b in left if not b & bit]))
        left = plan[-1][2]
        bit *= 2
    return plan


def kernel(
    groups, replicas, width,
    hs, gain, kw, vw, cosine, sine, deltas, outer, momentum, local,
    keys, values, momentum_new, outer_new, local_new,
    hs_v, gains, a_in, a_scaled, weights, inv, partial, d_in, o_in, *rest,
):
    plan = stage_plan(groups)
    stages = len(plan)
    c_out, c_in, rest = rest[:stages], rest[stages : 2 * stages], rest[2 * stages :]
    hs_sem, g_sem, a_sem, b_sem, own_sem, c_sem, d_sem, o_sem = rest

    r, f = lax.axis_index("replica"), lax.axis_index("fsdp")
    x, z = lax.rem(f, 2), lax.div(f, 2)
    tokens, depth = hs.shape[0], kw.shape[0]
    quarter = 2 * depth
    per_weight = kw.shape[1] // width
    chunks = 2 * per_weight
    own_w = outer.shape[1]

    def group_at(offset):
        g, bit = z, 1
        while bit < groups:
            if offset & bit:
                g = g + bit * (1 - 2 * lax.rem(lax.div(g, bit), 2))
            bit *= 2
        return g

    def peer(offset):
        return {"fsdp": 2 * group_at(offset) + x}

    partner = {"fsdp": f + 1 - 2 * x}

    def replica_at(j):
        return lax.rem(r + j, replicas)

    barrier = pltpu.get_barrier_semaphore()
    pl.semaphore_signal(barrier, inc=1, device_id=partner, device_id_type=MESH)
    for b in range(1, groups):
        pl.semaphore_signal(barrier, inc=1, device_id=peer(b), device_id_type=MESH)
    for j in range(1, replicas):
        pl.semaphore_signal(
            barrier, inc=1, device_id={"replica": replica_at(j)}, device_id_type=MESH
        )

    def remote(src, dst, sems, index, target):
        return pltpu.make_async_remote_copy(
            src_ref=src, dst_ref=dst, send_sem=sems.at[(0,) + index],
            recv_sem=sems.at[(1,) + index], device_id=target, device_id_type=MESH,
        )

    hs_copy = pltpu.make_async_copy(hs, hs_v, hs_sem)
    hs_copy.start()
    rows = pl.ds(pl.multiple_of(x * depth, depth), depth)
    own_copies = []
    for c in range(chunks):
        source = (kw if c < per_weight else vw).at[:, pl.ds((c % per_weight) * width, width)]
        own_copies.append(pltpu.make_async_copy(source, weights.at[c, rows], own_sem.at[c]))
        own_copies[-1].start()

    pl.semaphore_wait(barrier, groups + replicas - 1)

    gain_copy = remote(gain, gains.at[x], g_sem, (), partner)
    gain_copy.start()
    a_copies = {}

    def send_tokens(offsets):
        for b in offsets:
            columns = pl.ds(pl.multiple_of(group_at(b) * quarter, quarter), quarter)
            a_copies[b] = remote(hs.at[:, columns], a_in.at[b - 1], a_sem, (b - 1,), peer(b))
            a_copies[b].start()

    send_tokens(plan[0][1])
    b_copies = []
    for c in range(chunks):
        source = (kw if c < per_weight else vw).at[:, pl.ds((c % per_weight) * width, width)]
        b_copies.append(remote(source, weights.at[c, rows], b_sem, (c,), partner))
        b_copies[-1].start()
    d_copies = []
    for j in range(1, replicas):
        columns = pl.ds(pl.multiple_of(replica_at(j) * own_w, own_w), own_w)
        d_copies.append(
            remote(
                deltas.at[:, columns], d_in.at[j - 1], d_sem, (j - 1,), {"replica": replica_at(j)}
            )
        )
        d_copies[-1].start()

    def c_copy(stage, c):
        return remote(
            c_out[stage].at[c], c_in[stage].at[c], c_sem, (stage, c), peer(plan[stage][0])
        )

    def b_wait(c):
        pltpu.make_async_copy(
            kw.at[:, pl.ds(0, width)], weights.at[c, rows], own_sem.at[c]
        ).wait()
        remote(
            kw.at[:, pl.ds(0, width)], weights.at[c, rows], b_sem, (c,), partner
        ).wait_recv()

    hs_copy.wait()
    total = jnp.zeros((tokens, 1), jnp.float32)
    features = hs.shape[1]
    for k in range(groups):
        part = hs_v[:, k * quarter : (k + 1) * quarter].astype(jnp.float32)
        total += jnp.sum(part * part, axis=1, keepdims=True)
    inv[...] = jnp.broadcast_to(lax.rsqrt(total / features + 1e-05), inv.shape)

    gains[x] = gain[...]
    gain_copy.wait()
    gain_row = jnp.concatenate([gains[0], gains[1]], axis=1).astype(jnp.float32)

    def scale(b, block):
        a_scaled[b] = (block.astype(jnp.float32) * gain_row).astype(jnp.bfloat16)

    scale(0, hs_v[:, pl.ds(pl.multiple_of(z * quarter, quarter), quarter)])
    for b in plan[0][1]:
        a_copies[b].wait_recv()
        scale(b, a_in[b - 1])

    def product(b, c):
        return jnp.dot(a_scaled[b], weights[c], preferred_element_type=jnp.float32)

    def first_products(c):
        b_wait(c)
        for i, b in enumerate(plan[0][1]):
            c_out[0][c, i] = product(b, c).astype(jnp.bfloat16)
        c_copy(0, c).start()

    pl.loop(0, 1)(first_products)
    send_tokens([b for b in plan[0][2] if b])
    pl.loop(1, chunks)(first_products)

    avg = deltas[:, pl.ds(pl.multiple_of(r * own_w, own_w), own_w)]
    for j in range(1, replicas):
        d_copies[j - 1].wait_recv()
        avg += d_in[j - 1]
    avg = avg / replicas
    moved = 0.9 * momentum[...] + avg
    momentum_new[...] = moved
    outer_new[...] = outer[...] - 0.7 * (avg + 0.9 * moved)

    for b in plan[0][2]:
        if b:
            a_copies[b].wait_recv()
            scale(b, a_in[b - 1])

    o_copies = []
    for j in range(1, replicas):
        o_copies.append(
            remote(outer_new, o_in.at[j - 1], o_sem, (j - 1,), {"replica": replica_at(j)})
        )
        o_copies[-1].start()

    for stage in range(stages):
        bit, sent, kept = plan[stage]
        last = stage == stages - 1
        upcoming = [] if last else plan[stage + 1][1]

        def summed(b, c):
            before = product(b, c) if stage == 0 else partial[b, c]
            return before + c_in[stage][c, sent.index(b + bit)].astype(jnp.float32)

        if not last:

            @pl.loop(0, chunks)
            def _(c):
                c_copy(stage, c).wait_recv()
                for b in kept:
                    value = summed(b, c)
                    if b in upcoming:
                        c_out[stage + 1][c, upcoming.index(b)] = value.astype(jnp.bfloat16)
                    else:
                        partial[b, c] = value
                c_copy(stage + 1, c).start()

        if stage == 0:
            half = jnp.float32(0.5)
            mine = pl.ds(pl.multiple_of(r * own_w, own_w), own_w)
            local_new[:, mine] = (
                half * local[:, mine].astype(jnp.float32) + half * outer_new[...]
            ).astype(jnp.bfloat16)
            for j in range(1, replicas):
                o_copies[j - 1].wait_recv()
                theirs = pl.ds(
                    pl.multiple_of(lax.rem(r + replicas - j, replicas) * own_w, own_w), own_w
                )
                local_new[:, theirs] = (
                    half * local[:, theirs].astype(jnp.float32) + half * o_in[j - 1]
                ).astype(jnp.bfloat16)

        if last:

            @pl.loop(0, per_weight)
            def _(c):
                c_copy(stage, c).wait_recv()
                value = summed(0, c) * inv[:, 0:1]
                for h in range(width // HEAD):
                    head = value[:, h * HEAD : (h + 1) * HEAD]
                    turned = head * cosine[...] + pltpu.roll(head, HEAD // 2, 1) * sine[...]
                    at = pl.ds(pl.multiple_of(c * width + h * HEAD, HEAD), HEAD)
                    keys[:, at] = turned.astype(jnp.bfloat16)

            @pl.loop(0, per_weight)
            def _(c):
                c_copy(stage, c + per_weight).wait_recv()
                value = summed(0, c + per_weight) * inv[:, 0:1]
                at = pl.ds(pl.multiple_of(c * width, width), width)
                values[:, at] = value.astype(jnp.bfloat16)

    for copy in list(a_copies.values()) + b_copies + d_copies + o_copies:
        copy.wait_send()
    for stage in range(stages):

        @pl.loop(0, chunks)
        def _(c):
            c_copy(stage, c).wait_send()


def per_device(
    groups, replicas,
    hidden_states, norm_gain, key_weight, value_weight, deltas, outer_params, momentum, local_params,
):
    hs, kw, vw = hidden_states[0], key_weight[0], value_weight[0]
    tokens, features = hs.shape
    depth, kv = kw.shape
    width = 2 * HEAD
    chunks = 2 * kv // width
    cosine, sine = rotation_tables(tokens, HEAD)
    plan = stage_plan(groups)
    blocks = [pltpu.VMEM((chunks, len(p[1]), tokens, width), jnp.bfloat16) for p in plan]
    own = outer_params.shape
    vmem = pl.BlockSpec(memory_space=pltpu.VMEM)
    hbm = pl.BlockSpec(memory_space=pl.ANY)
    dma = pltpu.SemaphoreType.DMA
    results = pl.pallas_call(
        functools.partial(kernel, groups, replicas, width),
        out_shape=(
            jax.ShapeDtypeStruct((tokens, kv), jnp.bfloat16),
            jax.ShapeDtypeStruct((tokens, kv), jnp.bfloat16),
            jax.ShapeDtypeStruct(own, jnp.float32),
            jax.ShapeDtypeStruct(own, jnp.float32),
            jax.ShapeDtypeStruct(local_params.shape[1:], jnp.bfloat16),
        ),
        in_specs=[hbm, vmem, hbm, hbm] + [vmem] * 6,
        out_specs=[vmem] * 5,
        scratch_shapes=[
            pltpu.VMEM((tokens, features), jnp.bfloat16),
            pltpu.VMEM((2, 1, depth), jnp.bfloat16),
            pltpu.VMEM((groups - 1, tokens, 2 * depth), jnp.bfloat16),
            pltpu.VMEM((groups, tokens, 2 * depth), jnp.bfloat16),
            pltpu.VMEM((chunks, 2 * depth, width), jnp.bfloat16),
            pltpu.VMEM((tokens, HEAD), jnp.float32),
            pltpu.VMEM((max(p + 1 for p in plan[0][2] if not p & 2), chunks, tokens, width), jnp.float32),
            pltpu.VMEM((replicas - 1,) + own, jnp.float32),
            pltpu.VMEM((replicas - 1,) + own, jnp.float32),
            *blocks,
            *blocks,
            dma,
            dma((2,)),
            dma((2, groups - 1)),
            dma((2, chunks)),
            dma((chunks,)),
            dma((2, len(plan), chunks)),
            dma((2, replicas - 1)),
            dma((2, replicas - 1)),
        ],
        compiler_params=pltpu.CompilerParams(
            collective_id=0, has_side_effects=True, vmem_limit_bytes=60 * 1024 * 1024
        ),
    )(
        hs, norm_gain, kw, vw, cosine, sine,
        deltas[0], outer_params, momentum, local_params[0],
    )
    keys, values, momentum_new, outer_new, local_new = pl.pallas_call(
        write_out,
        out_shape=tuple(jax.ShapeDtypeStruct(a.shape, a.dtype) for a in results),
        in_specs=[hbm] * 5,
        out_specs=[hbm] * 5,
        scratch_shapes=[dma((5,))],
        compiler_params=pltpu.CompilerParams(vmem_limit_bytes=1024 * 1024),
    )(*results)
    return keys[None], values[None], momentum_new, outer_new, local_new[None]


def solution(mesh):
    in_specs = (
        P("replica", "fsdp", None),
        P("replica", "fsdp"),
        P("replica", "fsdp", None),
        P("replica", "fsdp", None),
        P("replica", "fsdp", None),
        P("fsdp", "replica"),
        P("fsdp", "replica"),
        P("replica", "fsdp", None),
    )
    out_specs = (
        P("replica", "fsdp", None),
        P("replica", "fsdp", None),
        P("fsdp", "replica"),
        P("fsdp", "replica"),
        P("replica", "fsdp", None),
    )
    groups, replicas = mesh.shape["fsdp"] // 2, mesh.shape["replica"]
    return jax.shard_map(
        functools.partial(per_device, groups, replicas),
        mesh=mesh, in_specs=in_specs, out_specs=out_specs, check_vma=False,
    )
```

```python
import functools

import jax
import jax.numpy as jnp
import numpy as np
from jax import lax
from jax.experimental import pallas as pl
from jax.experimental.pallas import tpu as pltpu
from jax.sharding import PartitionSpec as P

HEAD = 128
MESH = pl.DeviceIdType.MESH


def rotation_tables(tokens, head_size):
    half_width = head_size // 2
    exponent = np.arange(half_width, dtype=np.float32) * np.float32(2.0 / head_size)
    frequency = np.power(np.float32(500000.0), -exponent)
    angles = np.arange(tokens, dtype=np.float32)[:, None] * frequency[None, :]
    cosine, sine = np.cos(angles), np.sin(angles)
    return (
        jnp.asarray(np.concatenate([cosine, cosine], axis=1)),
        jnp.asarray(np.concatenate([-sine, sine], axis=1)),
    )


def write_out(*refs):
    count = len(refs) // 2
    sems = refs[-1]
    copies = [
        pltpu.make_async_copy(refs[i], refs[count + i], sems.at[i]) for i in range(count)
    ]
    for copy in copies:
        copy.start()
    for copy in copies:
        copy.wait()


def stage_plan(groups):
    plan, left, bit = [], list(range(groups)), 1
    while bit < groups:
        plan.append((bit, [b for b in left if b & bit], [b for b in left if not b & bit]))
        left = plan[-1][2]
        bit *= 2
    return plan


def kernel(
    groups, replicas, width,
    hs, gain, kw, vw, cosine_in, sine_in, deltas, outer_in, momentum_in, local_in,
    keys_out, values_out, momentum_out, outer_out, local_out,
    cosine, sine, deltas_own, outer, momentum, local,
    keys, values, momentum_new, outer_new, local_new,
    hs_v, gains, a_in, a_scaled, weights, inv, partial, d_in, o_in, *rest,
):
    plan = stage_plan(groups)
    stages = len(plan)
    c_out, c_in, rest = rest[:stages], rest[stages : 2 * stages], rest[2 * stages :]
    hs_sem, g_sem, a_sem, b_sem, own_sem, c_sem, d_sem, o_sem, load_sem, store_sem = rest

    r, f = lax.axis_index("replica"), lax.axis_index("fsdp")
    x, z = lax.rem(f, 2), lax.div(f, 2)
    tokens, depth = hs.shape[0], kw.shape[0]
    quarter = 2 * depth
    per_weight = kw.shape[1] // width
    chunks = 2 * per_weight
    own_w = outer.shape[1]

    def group_at(offset):
        g, bit = z, 1
        while bit < groups:
            if offset & bit:
                g = g + bit * (1 - 2 * lax.rem(lax.div(g, bit), 2))
            bit *= 2
        return g

    def peer(offset):
        return {"fsdp": 2 * group_at(offset) + x}

    partner = {"fsdp": f + 1 - 2 * x}

    def replica_at(j):
        return lax.rem(r + j, replicas)

    barrier = pltpu.get_barrier_semaphore()
    pl.semaphore_signal(barrier, inc=1, device_id=partner, device_id_type=MESH)
    for b in range(1, groups):
        pl.semaphore_signal(barrier, inc=1, device_id=peer(b), device_id_type=MESH)
    for j in range(1, replicas):
        pl.semaphore_signal(
            barrier, inc=1, device_id={"replica": replica_at(j)}, device_id_type=MESH
        )

    def remote(src, dst, sems, index, target):
        return pltpu.make_async_remote_copy(
            src_ref=src, dst_ref=dst, send_sem=sems.at[(0,) + index],
            recv_sem=sems.at[(1,) + index], device_id=target, device_id_type=MESH,
        )

    mine = pl.ds(pl.multiple_of(r * own_w, own_w), own_w)
    hs_copy = pltpu.make_async_copy(hs, hs_v, hs_sem)
    hs_copy.start()
    loads = [
        pltpu.make_async_copy(source, target, load_sem.at[i])
        for i, (source, target) in enumerate(
            (
                (deltas.at[:, mine], deltas_own),
                (outer_in, outer),
                (momentum_in, momentum),
                (local_in, local),
                (cosine_in, cosine),
                (sine_in, sine),
            )
        )
    ]
    rows = pl.ds(pl.multiple_of(x * depth, depth), depth)
    own_copies = []
    for c in range(chunks):
        source = (kw if c < per_weight else vw).at[:, pl.ds((c % per_weight) * width, width)]
        own_copies.append(pltpu.make_async_copy(source, weights.at[c, rows], own_sem.at[c]))
        own_copies[-1].start()

    pl.semaphore_wait(barrier, groups + replicas - 1)

    gain_copy = remote(gain, gains.at[x], g_sem, (), partner)
    gain_copy.start()
    a_copies = {}

    def send_tokens(offsets):
        for b in offsets:
            columns = pl.ds(pl.multiple_of(group_at(b) * quarter, quarter), quarter)
            a_copies[b] = remote(hs.at[:, columns], a_in.at[b - 1], a_sem, (b - 1,), peer(b))
            a_copies[b].start()

    send_tokens(plan[0][1])
    b_copies = []
    for c in range(chunks):
        source = (kw if c < per_weight else vw).at[:, pl.ds((c % per_weight) * width, width)]
        b_copies.append(remote(source, weights.at[c, rows], b_sem, (c,), partner))
        b_copies[-1].start()
    d_copies = []
    for j in range(1, replicas):
        columns = pl.ds(pl.multiple_of(replica_at(j) * own_w, own_w), own_w)
        d_copies.append(
            remote(
                deltas.at[:, columns], d_in.at[j - 1], d_sem, (j - 1,), {"replica": replica_at(j)}
            )
        )
        d_copies[-1].start()

    for copy in loads:
        copy.start()

    def store(i, source, target):
        copy = pltpu.make_async_copy(source, target, store_sem.at[i])
        copy.start()
        return copy

    def result_copy(source, target, c, sem):
        at = pl.ds(pl.multiple_of(c * width, width), width)
        return pltpu.make_async_copy(source.at[:, at], target.at[:, at], store_sem.at[sem])

    def c_copy(stage, c):
        return remote(
            c_out[stage].at[c], c_in[stage].at[c], c_sem, (stage, c), peer(plan[stage][0])
        )

    def b_wait(c):
        pltpu.make_async_copy(
            kw.at[:, pl.ds(0, width)], weights.at[c, rows], own_sem.at[c]
        ).wait()
        remote(
            kw.at[:, pl.ds(0, width)], weights.at[c, rows], b_sem, (c,), partner
        ).wait_recv()

    hs_copy.wait()
    total = jnp.zeros((tokens, 1), jnp.float32)
    features = hs.shape[1]
    for k in range(groups):
        part = hs_v[:, k * quarter : (k + 1) * quarter].astype(jnp.float32)
        total += jnp.sum(part * part, axis=1, keepdims=True)
    inv[...] = jnp.broadcast_to(lax.rsqrt(total / features + 1e-05), inv.shape)

    gains[x] = gain[...]
    gain_copy.wait()
    gain_row = jnp.concatenate([gains[0], gains[1]], axis=1).astype(jnp.float32)

    def scale(b, block):
        a_scaled[b] = (block.astype(jnp.float32) * gain_row).astype(jnp.bfloat16)

    scale(0, hs_v[:, pl.ds(pl.multiple_of(z * quarter, quarter), quarter)])
    for b in plan[0][1]:
        a_copies[b].wait_recv()
        scale(b, a_in[b - 1])

    def product(b, c):
        return jnp.dot(a_scaled[b], weights[c], preferred_element_type=jnp.float32)

    def first_products(c):
        b_wait(c)
        for i, b in enumerate(plan[0][1]):
            c_out[0][c, i] = product(b, c).astype(jnp.bfloat16)
        c_copy(0, c).start()

    pl.loop(0, 1)(first_products)
    send_tokens([b for b in plan[0][2] if b])
    pl.loop(1, chunks)(first_products)

    for copy in loads:
        copy.wait()
    avg = deltas_own[...]
    for j in range(1, replicas):
        d_copies[j - 1].wait_recv()
        avg += d_in[j - 1]
    avg = avg / replicas
    moved = 0.9 * momentum[...] + avg
    momentum_new[...] = moved
    outer_new[...] = outer[...] - 0.7 * (avg + 0.9 * moved)
    stores = [store(0, momentum_new, momentum_out), store(1, outer_new, outer_out)]

    for b in plan[0][2]:
        if b:
            a_copies[b].wait_recv()
            scale(b, a_in[b - 1])

    o_copies = []
    for j in range(1, replicas):
        o_copies.append(
            remote(outer_new, o_in.at[j - 1], o_sem, (j - 1,), {"replica": replica_at(j)})
        )
        o_copies[-1].start()

    for stage in range(stages):
        bit, sent, kept = plan[stage]
        last = stage == stages - 1
        upcoming = [] if last else plan[stage + 1][1]

        def summed(b, c):
            before = product(b, c) if stage == 0 else partial[b, c]
            return before + c_in[stage][c, sent.index(b + bit)].astype(jnp.float32)

        if not last:

            @pl.loop(0, chunks)
            def _(c):
                c_copy(stage, c).wait_recv()
                for b in kept:
                    value = summed(b, c)
                    if b in upcoming:
                        c_out[stage + 1][c, upcoming.index(b)] = value.astype(jnp.bfloat16)
                    else:
                        partial[b, c] = value
                c_copy(stage + 1, c).start()

        if stage == 0:
            half = jnp.float32(0.5)
            local_new[:, mine] = (
                half * local[:, mine].astype(jnp.float32) + half * outer_new[...]
            ).astype(jnp.bfloat16)
            for j in range(1, replicas):
                o_copies[j - 1].wait_recv()
                theirs = pl.ds(
                    pl.multiple_of(lax.rem(r + replicas - j, replicas) * own_w, own_w), own_w
                )
                local_new[:, theirs] = (
                    half * local[:, theirs].astype(jnp.float32) + half * o_in[j - 1]
                ).astype(jnp.bfloat16)
            stores.append(store(2, local_new, local_out))

        if last:

            @pl.loop(0, per_weight)
            def _(c):
                c_copy(stage, c).wait_recv()
                value = summed(0, c) * inv[:, 0:1]
                for h in range(width // HEAD):
                    head = value[:, h * HEAD : (h + 1) * HEAD]
                    turned = head * cosine[...] + pltpu.roll(head, HEAD // 2, 1) * sine[...]
                    at = pl.ds(pl.multiple_of(c * width + h * HEAD, HEAD), HEAD)
                    keys[:, at] = turned.astype(jnp.bfloat16)
                result_copy(keys, keys_out, c, 3 + c).start()

            @pl.loop(0, per_weight)
            def _(c):
                c_copy(stage, c + per_weight).wait_recv()
                value = summed(0, c + per_weight) * inv[:, 0:1]
                at = pl.ds(pl.multiple_of(c * width, width), width)
                values[:, at] = value.astype(jnp.bfloat16)
                result_copy(values, values_out, c, 3 + per_weight + c).start()

    for copy in stores:
        copy.wait()

    @pl.loop(0, per_weight)
    def _(c):
        result_copy(keys, keys_out, c, 3 + c).wait()
        result_copy(values, values_out, c, 3 + per_weight + c).wait()

    for copy in list(a_copies.values()) + b_copies + d_copies + o_copies:
        copy.wait_send()
    for stage in range(stages):

        @pl.loop(0, chunks)
        def _(c):
            c_copy(stage, c).wait_send()


def per_device(
    groups, replicas,
    hidden_states, norm_gain, key_weight, value_weight, deltas, outer_params, momentum, local_params,
):
    hs, kw, vw = hidden_states[0], key_weight[0], value_weight[0]
    tokens, features = hs.shape
    depth, kv = kw.shape
    width = 2 * HEAD
    chunks = 2 * kv // width
    cosine, sine = rotation_tables(tokens, HEAD)
    plan = stage_plan(groups)
    blocks = [pltpu.VMEM((chunks, len(p[1]), tokens, width), jnp.bfloat16) for p in plan]
    own = outer_params.shape
    vmem = pl.BlockSpec(memory_space=pltpu.VMEM)
    hbm = pl.BlockSpec(memory_space=pl.ANY)
    dma = pltpu.SemaphoreType.DMA
    results = pl.pallas_call(
        functools.partial(kernel, groups, replicas, width),
        out_shape=(
            jax.ShapeDtypeStruct((tokens, kv), jnp.bfloat16),
            jax.ShapeDtypeStruct((tokens, kv), jnp.bfloat16),
            jax.ShapeDtypeStruct(own, jnp.float32),
            jax.ShapeDtypeStruct(own, jnp.float32),
            jax.ShapeDtypeStruct(local_params.shape[1:], jnp.bfloat16),
        ),
        in_specs=[hbm, vmem] + [hbm] * 8,
        out_specs=[hbm] * 5,
        scratch_shapes=[
            pltpu.VMEM(cosine.shape, jnp.float32),
            pltpu.VMEM(sine.shape, jnp.float32),
            pltpu.VMEM(own, jnp.float32),
            pltpu.VMEM(own, jnp.float32),
            pltpu.VMEM(own, jnp.float32),
            pltpu.VMEM(local_params.shape[1:], jnp.bfloat16),
            pltpu.VMEM((tokens, kv), jnp.bfloat16),
            pltpu.VMEM((tokens, kv), jnp.bfloat16),
            pltpu.VMEM(own, jnp.float32),
            pltpu.VMEM(own, jnp.float32),
            pltpu.VMEM(local_params.shape[1:], jnp.bfloat16),
            pltpu.VMEM((tokens, features), jnp.bfloat16),
            pltpu.VMEM((2, 1, depth), jnp.bfloat16),
            pltpu.VMEM((groups - 1, tokens, 2 * depth), jnp.bfloat16),
            pltpu.VMEM((groups, tokens, 2 * depth), jnp.bfloat16),
            pltpu.VMEM((chunks, 2 * depth, width), jnp.bfloat16),
            pltpu.VMEM((tokens, HEAD), jnp.float32),
            pltpu.VMEM((max(p + 1 for p in plan[0][2] if not p & 2), chunks, tokens, width), jnp.float32),
            pltpu.VMEM((replicas - 1,) + own, jnp.float32),
            pltpu.VMEM((replicas - 1,) + own, jnp.float32),
            *blocks,
            *blocks,
            dma,
            dma((2,)),
            dma((2, groups - 1)),
            dma((2, chunks)),
            dma((chunks,)),
            dma((2, len(plan), chunks)),
            dma((2, replicas - 1)),
            dma((2, replicas - 1)),
            dma((6,)),
            dma((3 + chunks,)),
        ],
        compiler_params=pltpu.CompilerParams(
            collective_id=0, has_side_effects=True, vmem_limit_bytes=60 * 1024 * 1024
        ),
    )(
        hs, norm_gain, kw, vw, cosine, sine,
        deltas[0], outer_params, momentum, local_params[0],
    )
    keys, values, momentum_new, outer_new, local_new = pl.pallas_call(
        write_out,
        out_shape=tuple(jax.ShapeDtypeStruct(a.shape, a.dtype) for a in results),
        in_specs=[vmem] * 5,
        out_specs=[hbm] * 5,
        scratch_shapes=[dma((5,))],
        compiler_params=pltpu.CompilerParams(vmem_limit_bytes=60 * 1024 * 1024),
    )(*results)
    return keys[None], values[None], momentum_new, outer_new, local_new[None]


def solution(mesh):
    in_specs = (
        P("replica", "fsdp", None),
        P("replica", "fsdp"),
        P("replica", "fsdp", None),
        P("replica", "fsdp", None),
        P("replica", "fsdp", None),
        P("fsdp", "replica"),
        P("fsdp", "replica"),
        P("replica", "fsdp", None),
    )
    out_specs = (
        P("replica", "fsdp", None),
        P("replica", "fsdp", None),
        P("fsdp", "replica"),
        P("fsdp", "replica"),
        P("replica", "fsdp", None),
    )
    groups, replicas = mesh.shape["fsdp"] // 2, mesh.shape["replica"]
    return jax.shard_map(
        functools.partial(per_device, groups, replicas),
        mesh=mesh, in_specs=in_specs, out_specs=out_specs, check_vma=False,
    )
```

```python
import functools

import jax
import jax.numpy as jnp
import numpy as np
from jax import lax
from jax.experimental import pallas as pl
from jax.experimental.pallas import tpu as pltpu
from jax.sharding import PartitionSpec as P

HEAD = 128
MESH = pl.DeviceIdType.MESH


def rotation_tables(tokens, head_size):
    half_width = head_size // 2
    exponent = np.arange(half_width, dtype=np.float32) * np.float32(2.0 / head_size)
    frequency = np.power(np.float32(500000.0), -exponent)
    angles = np.arange(tokens, dtype=np.float32)[:, None] * frequency[None, :]
    cosine, sine = np.cos(angles), np.sin(angles)
    return (
        jnp.asarray(np.concatenate([cosine, cosine], axis=1)),
        jnp.asarray(np.concatenate([-sine, sine], axis=1)),
    )


def write_out(*refs):
    count = len(refs) // 2
    sems = refs[-1]
    copies = [
        pltpu.make_async_copy(refs[i], refs[count + i], sems.at[i]) for i in range(count)
    ]
    for copy in copies:
        copy.start()
    for copy in copies:
        copy.wait()


def stage_plan(groups):
    plan, left, bit = [], list(range(groups)), 1
    while bit < groups:
        plan.append((bit, [b for b in left if b & bit], [b for b in left if not b & bit]))
        left = plan[-1][2]
        bit *= 2
    return plan


def kernel(
    groups, replicas, width,
    hs, gain, kw, vw, cosine_in, sine_in, deltas, outer_in, momentum_in, local_in,
    keys_out, values_out, momentum_out, outer_out, local_out,
    cosine, sine, deltas_own, outer, momentum, local,
    keys, values, momentum_new, outer_new, local_new,
    hs_v, gains, a_in, a_scaled, weights, inv, partial, d_in, o_in, *rest,
):
    plan = stage_plan(groups)
    stages = len(plan)
    c_out, c_in, rest = rest[:stages], rest[stages : 2 * stages], rest[2 * stages :]
    hs_sem, g_sem, a_sem, b_sem, own_sem, c_sem, d_sem, o_sem, load_sem, store_sem = rest

    r, f = lax.axis_index("replica"), lax.axis_index("fsdp")
    x, z = lax.rem(f, 2), lax.div(f, 2)
    tokens, depth = hs.shape[0], kw.shape[0]
    quarter = 2 * depth
    per_weight = kw.shape[1] // width
    chunks = 2 * per_weight
    own_w = outer.shape[1]

    def group_at(offset):
        g, bit = z, 1
        while bit < groups:
            if offset & bit:
                g = g + bit * (1 - 2 * lax.rem(lax.div(g, bit), 2))
            bit *= 2
        return g

    def peer(offset):
        return {"fsdp": 2 * group_at(offset) + x}

    partner = {"fsdp": f + 1 - 2 * x}

    def replica_at(j):
        return lax.rem(r + j, replicas)

    barrier = pltpu.get_barrier_semaphore()
    pl.semaphore_signal(barrier, inc=1, device_id=partner, device_id_type=MESH)
    for b in range(1, groups):
        pl.semaphore_signal(barrier, inc=1, device_id=peer(b), device_id_type=MESH)
    for j in range(1, replicas):
        pl.semaphore_signal(
            barrier, inc=1, device_id={"replica": replica_at(j)}, device_id_type=MESH
        )

    def remote(src, dst, sems, index, target):
        return pltpu.make_async_remote_copy(
            src_ref=src, dst_ref=dst, send_sem=sems.at[(0,) + index],
            recv_sem=sems.at[(1,) + index], device_id=target, device_id_type=MESH,
        )

    mine = pl.ds(pl.multiple_of(r * own_w, own_w), own_w)
    hs_copy = pltpu.make_async_copy(hs, hs_v, hs_sem)
    hs_copy.start()
    loads = [
        pltpu.make_async_copy(source, target, load_sem.at[i])
        for i, (source, target) in enumerate(
            (
                (deltas.at[:, mine], deltas_own),
                (outer_in, outer),
                (momentum_in, momentum),
                (local_in, local),
                (cosine_in, cosine),
                (sine_in, sine),
            )
        )
    ]
    rows = pl.ds(pl.multiple_of(x * depth, depth), depth)
    own_copies = []
    for c in range(chunks):
        source = (kw if c < per_weight else vw).at[:, pl.ds((c % per_weight) * width, width)]
        own_copies.append(pltpu.make_async_copy(source, weights.at[c, rows], own_sem.at[c]))
        own_copies[-1].start()

    pl.semaphore_wait(barrier, groups + replicas - 1)

    gain_copy = remote(gain, gains.at[x], g_sem, (), partner)
    gain_copy.start()
    a_copies = {}

    def send_tokens(offsets):
        for b in offsets:
            columns = pl.ds(pl.multiple_of(group_at(b) * quarter, quarter), quarter)
            a_copies[b] = remote(hs.at[:, columns], a_in.at[b - 1], a_sem, (b - 1,), peer(b))
            a_copies[b].start()

    send_tokens(plan[0][1][::-1] + [b for b in plan[0][2] if b])
    b_copies = []
    for c in range(chunks):
        source = (kw if c < per_weight else vw).at[:, pl.ds((c % per_weight) * width, width)]
        b_copies.append(remote(source, weights.at[c, rows], b_sem, (c,), partner))
        b_copies[-1].start()
    d_copies = []
    for j in range(1, replicas):
        columns = pl.ds(pl.multiple_of(replica_at(j) * own_w, own_w), own_w)
        d_copies.append(
            remote(
                deltas.at[:, columns], d_in.at[j - 1], d_sem, (j - 1,), {"replica": replica_at(j)}
            )
        )
        d_copies[-1].start()

    for copy in loads:
        copy.start()

    def store(i, source, target):
        copy = pltpu.make_async_copy(source, target, store_sem.at[i])
        copy.start()
        return copy

    def result_copy(source, target, c, sem):
        at = pl.ds(pl.multiple_of(c * width, width), width)
        return pltpu.make_async_copy(source.at[:, at], target.at[:, at], store_sem.at[sem])

    def c_copy(stage, c):
        return remote(
            c_out[stage].at[c], c_in[stage].at[c], c_sem, (stage, c), peer(plan[stage][0])
        )

    def b_wait(c):
        pltpu.make_async_copy(
            kw.at[:, pl.ds(0, width)], weights.at[c, rows], own_sem.at[c]
        ).wait()
        remote(
            kw.at[:, pl.ds(0, width)], weights.at[c, rows], b_sem, (c,), partner
        ).wait_recv()

    hs_copy.wait()
    total = jnp.zeros((tokens, 1), jnp.float32)
    features = hs.shape[1]
    for k in range(groups):
        part = hs_v[:, k * quarter : (k + 1) * quarter].astype(jnp.float32)
        total += jnp.sum(part * part, axis=1, keepdims=True)
    inv[...] = jnp.broadcast_to(lax.rsqrt(total / features + 1e-05), inv.shape)

    gains[x] = gain[...]
    gain_copy.wait()
    gain_row = jnp.concatenate([gains[0], gains[1]], axis=1).astype(jnp.float32)

    def scale(b, block):
        a_scaled[b] = (block.astype(jnp.float32) * gain_row).astype(jnp.bfloat16)

    scale(0, hs_v[:, pl.ds(pl.multiple_of(z * quarter, quarter), quarter)])
    for b in plan[0][1]:
        a_copies[b].wait_recv()
        scale(b, a_in[b - 1])

    def product(b, c):
        return jnp.dot(a_scaled[b], weights[c], preferred_element_type=jnp.float32)

    def first_products(c):
        b_wait(c)
        for i, b in enumerate(plan[0][1]):
            c_out[0][c, i] = product(b, c).astype(jnp.bfloat16)
        c_copy(0, c).start()

    pl.loop(0, chunks)(first_products)

    for copy in loads:
        copy.wait()
    avg = deltas_own[...]
    for j in range(1, replicas):
        d_copies[j - 1].wait_recv()
        avg += d_in[j - 1]
    avg = avg / replicas
    moved = 0.9 * momentum[...] + avg
    momentum_new[...] = moved
    outer_new[...] = outer[...] - 0.7 * (avg + 0.9 * moved)
    stores = [store(0, momentum_new, momentum_out), store(1, outer_new, outer_out)]

    for b in plan[0][2]:
        if b:
            a_copies[b].wait_recv()
            scale(b, a_in[b - 1])

    o_copies = []
    for j in range(1, replicas):
        o_copies.append(
            remote(outer_new, o_in.at[j - 1], o_sem, (j - 1,), {"replica": replica_at(j)})
        )
        o_copies[-1].start()

    for stage in range(stages):
        bit, sent, kept = plan[stage]
        last = stage == stages - 1
        upcoming = [] if last else plan[stage + 1][1]

        def summed(b, c):
            before = product(b, c) if stage == 0 else partial[b, c]
            return before + c_in[stage][c, sent.index(b + bit)].astype(jnp.float32)

        if not last:

            @pl.loop(0, chunks)
            def _(c):
                c_copy(stage, c).wait_recv()
                for b in kept:
                    value = summed(b, c)
                    if b in upcoming:
                        c_out[stage + 1][c, upcoming.index(b)] = value.astype(jnp.bfloat16)
                    else:
                        partial[b, c] = value
                c_copy(stage + 1, c).start()

        if stage == 0:
            half = jnp.float32(0.5)
            local_new[:, mine] = (
                half * local[:, mine].astype(jnp.float32) + half * outer_new[...]
            ).astype(jnp.bfloat16)
            for j in range(1, replicas):
                o_copies[j - 1].wait_recv()
                theirs = pl.ds(
                    pl.multiple_of(lax.rem(r + replicas - j, replicas) * own_w, own_w), own_w
                )
                local_new[:, theirs] = (
                    half * local[:, theirs].astype(jnp.float32) + half * o_in[j - 1]
                ).astype(jnp.bfloat16)
            stores.append(store(2, local_new, local_out))

        if last:

            @pl.loop(0, per_weight)
            def _(c):
                c_copy(stage, c).wait_recv()
                value = summed(0, c) * inv[:, 0:1]
                for h in range(width // HEAD):
                    head = value[:, h * HEAD : (h + 1) * HEAD]
                    turned = head * cosine[...] + pltpu.roll(head, HEAD // 2, 1) * sine[...]
                    at = pl.ds(pl.multiple_of(c * width + h * HEAD, HEAD), HEAD)
                    keys[:, at] = turned.astype(jnp.bfloat16)
                result_copy(keys, keys_out, c, 3 + c).start()

            @pl.loop(0, per_weight)
            def _(c):
                c_copy(stage, c + per_weight).wait_recv()
                value = summed(0, c + per_weight) * inv[:, 0:1]
                at = pl.ds(pl.multiple_of(c * width, width), width)
                values[:, at] = value.astype(jnp.bfloat16)
                result_copy(values, values_out, c, 3 + per_weight + c).start()

    for copy in stores:
        copy.wait()

    @pl.loop(0, per_weight)
    def _(c):
        result_copy(keys, keys_out, c, 3 + c).wait()
        result_copy(values, values_out, c, 3 + per_weight + c).wait()

    for copy in list(a_copies.values()) + b_copies + d_copies + o_copies:
        copy.wait_send()
    for stage in range(stages):

        @pl.loop(0, chunks)
        def _(c):
            c_copy(stage, c).wait_send()


def per_device(
    groups, replicas,
    hidden_states, norm_gain, key_weight, value_weight, deltas, outer_params, momentum, local_params,
):
    hs, kw, vw = hidden_states[0], key_weight[0], value_weight[0]
    tokens, features = hs.shape
    depth, kv = kw.shape
    width = 2 * HEAD
    chunks = 2 * kv // width
    cosine, sine = rotation_tables(tokens, HEAD)
    plan = stage_plan(groups)
    blocks = [pltpu.VMEM((chunks, len(p[1]), tokens, width), jnp.bfloat16) for p in plan]
    own = outer_params.shape
    vmem = pl.BlockSpec(memory_space=pltpu.VMEM)
    hbm = pl.BlockSpec(memory_space=pl.ANY)
    dma = pltpu.SemaphoreType.DMA
    results = pl.pallas_call(
        functools.partial(kernel, groups, replicas, width),
        out_shape=(
            jax.ShapeDtypeStruct((tokens, kv), jnp.bfloat16),
            jax.ShapeDtypeStruct((tokens, kv), jnp.bfloat16),
            jax.ShapeDtypeStruct(own, jnp.float32),
            jax.ShapeDtypeStruct(own, jnp.float32),
            jax.ShapeDtypeStruct(local_params.shape[1:], jnp.bfloat16),
        ),
        in_specs=[hbm, vmem] + [hbm] * 8,
        out_specs=[hbm] * 5,
        scratch_shapes=[
            pltpu.VMEM(cosine.shape, jnp.float32),
            pltpu.VMEM(sine.shape, jnp.float32),
            pltpu.VMEM(own, jnp.float32),
            pltpu.VMEM(own, jnp.float32),
            pltpu.VMEM(own, jnp.float32),
            pltpu.VMEM(local_params.shape[1:], jnp.bfloat16),
            pltpu.VMEM((tokens, kv), jnp.bfloat16),
            pltpu.VMEM((tokens, kv), jnp.bfloat16),
            pltpu.VMEM(own, jnp.float32),
            pltpu.VMEM(own, jnp.float32),
            pltpu.VMEM(local_params.shape[1:], jnp.bfloat16),
            pltpu.VMEM((tokens, features), jnp.bfloat16),
            pltpu.VMEM((2, 1, depth), jnp.bfloat16),
            pltpu.VMEM((groups - 1, tokens, 2 * depth), jnp.bfloat16),
            pltpu.VMEM((groups, tokens, 2 * depth), jnp.bfloat16),
            pltpu.VMEM((chunks, 2 * depth, width), jnp.bfloat16),
            pltpu.VMEM((tokens, HEAD), jnp.float32),
            pltpu.VMEM((max(p + 1 for p in plan[0][2] if not p & 2), chunks, tokens, width), jnp.float32),
            pltpu.VMEM((replicas - 1,) + own, jnp.float32),
            pltpu.VMEM((replicas - 1,) + own, jnp.float32),
            *blocks,
            *blocks,
            dma,
            dma((2,)),
            dma((2, groups - 1)),
            dma((2, chunks)),
            dma((chunks,)),
            dma((2, len(plan), chunks)),
            dma((2, replicas - 1)),
            dma((2, replicas - 1)),
            dma((6,)),
            dma((3 + chunks,)),
        ],
        compiler_params=pltpu.CompilerParams(
            collective_id=0, has_side_effects=True, vmem_limit_bytes=60 * 1024 * 1024
        ),
    )(
        hs, norm_gain, kw, vw, cosine, sine,
        deltas[0], outer_params, momentum, local_params[0],
    )
    keys, values, momentum_new, outer_new, local_new = pl.pallas_call(
        write_out,
        out_shape=tuple(jax.ShapeDtypeStruct(a.shape, a.dtype) for a in results),
        in_specs=[vmem] * 5,
        out_specs=[hbm] * 5,
        scratch_shapes=[dma((5,))],
        compiler_params=pltpu.CompilerParams(vmem_limit_bytes=60 * 1024 * 1024),
    )(*results)
    return keys[None], values[None], momentum_new, outer_new, local_new[None]


def solution(mesh):
    in_specs = (
        P("replica", "fsdp", None),
        P("replica", "fsdp"),
        P("replica", "fsdp", None),
        P("replica", "fsdp", None),
        P("replica", "fsdp", None),
        P("fsdp", "replica"),
        P("fsdp", "replica"),
        P("replica", "fsdp", None),
    )
    out_specs = (
        P("replica", "fsdp", None),
        P("replica", "fsdp", None),
        P("fsdp", "replica"),
        P("fsdp", "replica"),
        P("replica", "fsdp", None),
    )
    groups, replicas = mesh.shape["fsdp"] // 2, mesh.shape["replica"]
    return jax.shard_map(
        functools.partial(per_device, groups, replicas),
        mesh=mesh, in_specs=in_specs, out_specs=out_specs, check_vma=False,
    )
```
